32 devices in a mesh: dp: 8 (over z, x), tensor: 4 (over y, core).
Axes of the slice: x: 2, y: 2, z: 4, core: 2. Of those that a mesh axis runs over, the one named last changes fastest.
Arguments:
- out_grad: bfloat16 [1536, 2048], P(('dp', 'tensor')), may hold values from -6 to 6
- gate_pre: bfloat16 [1536, 7168], P('dp', 'tensor'), may hold values from -6 to 6
- up_pre: bfloat16 [1536, 7168], P('dp', 'tensor'), may hold values from -6 to 6
- down_weight: bfloat16 [7168, 2048], P('tensor', 'dp'), may hold values from -0.0625 to 0.0625
- up_weight: bfloat16 [2048, 7168], P('dp', 'tensor'), may hold values from -0.125 to 0.125
Outputs:
- input_grad: bfloat16 [1536, 2048], P(('dp', 'tensor'))
- gate_grad: bfloat16 [1536, 7168], P('dp', 'tensor')
- down_grad_t: float32 [2048, 7168], P('dp', 'tensor')
The draws below stay inside these ranges and needn't reach their ends.
All inputs are finite; a program needn't handle non-finite values.
Results may differ from the reference program's by a relative error of at most 0.009.
Values may be sent and summed in bfloat16 or wider, within the bound.
No kernel may reach another device: no remote copies, remote signals or barrier semaphores. Data moves between devices by JAX's collectives and lax.ppermute only.
A program may use at most 128 MiB of HBM per device.

```python
import jax
import jax.numpy as jnp
from jax import lax

D = 2048
FF = 7168
TOK_DEV = 48
TOKENS = 1536
N_DP = 8
N_TENSOR = 4


def raised(result, own_key, source, target, blocks, factor):
    def block_of(dim):
        return (jnp.arange(result.shape[dim]) // (result.shape[dim] // blocks)).reshape((-1,) + (1,) * (result.ndim - 1 - dim))

    one_side = jax.random.permutation(own_key, blocks)[block_of(target)]
    second = (block_of(target) + blocks // 2) % blocks
    return jnp.where((block_of(source) == one_side) | (block_of(source) == second), factor * result, result)


def block_levels(rng, dims, cuts, smallest, high):
    gain, own = 1.0, jax.random.fold_in(rng, 6)
    for dim, blocks in cuts:
        draws = jnp.exp(jax.random.uniform(jax.random.fold_in(own, dim), (blocks,), jnp.float32, smallest / len(cuts), high / len(cuts)))
        gain = gain * jnp.repeat(draws, dims[dim] // blocks).reshape([-1 if axis == dim else 1 for axis in range(len(dims))])
    return gain


def bell_draw(rng, extent, width, most, pieces=(), held_as=jnp.bfloat16):
    result = jax.random.normal(rng, extent, jnp.float32) * width
    if len(pieces) > 0:
        result = block_levels(rng, extent, pieces, -0.22, 0.18) * result
    return jnp.clip(result, min=-most, max=most).astype(held_as)


def bell_draw_with(rng, extent, spread, most, shards, heavy, dtype=jnp.bfloat16):
    array = spread * jax.random.normal(rng, extent, jnp.float32)
    if shards:
        array = array * block_levels(rng, extent, shards, -0.22, 0.18)
    return jnp.clip(raised(array, jax.random.fold_in(rng, 3), *heavy), -most, most).astype(dtype)


def setup_inputs(seed: int = 0) -> dict:
    arg_keys = jax.random.split(jax.random.key(seed), 6)
    out_grad = bell_draw_with(arg_keys[0], (TOKENS, D), 1.0, 6.0, ((0, 32),), (0, 1, 32, 2.75))
    gate_pre = bell_draw(arg_keys[1], (TOKENS, FF), 1.0, 6.0, ((0, 8), (1, 4)))
    up_pre = bell_draw(arg_keys[2], (TOKENS, FF), 1.0, 6.0, ((0, 8), (1, 4)))
    down_weight = bell_draw(arg_keys[3], (FF, D), FF ** -0.5, 0.0625, ((0, 4), (1, 8)))
    up_weight = bell_draw(arg_keys[4], (D, FF), D ** -0.5, 0.125, ((0, 8), (1, 4)))
    return {"out_grad": out_grad, "gate_pre": gate_pre, "up_pre": up_pre, "down_weight": down_weight, "up_weight": up_weight}


def reference(out_grad, gate_pre, up_pre, down_weight, up_weight):
    per_group = TOK_DEV * N_TENSOR
    slices = FF // N_TENSOR
    dy_blocks = out_grad.reshape(N_DP, per_group, D)
    gate_blocks = gate_pre.reshape(N_DP, per_group, FF)
    up_blocks = up_pre.reshape(N_DP, per_group, FF)
    up_split = up_weight.astype(jnp.float32).reshape(D, N_TENSOR, slices)

    def one_group(accum, blocks):
        dy_block, gate_block, up_block = blocks
        upstream = jnp.dot(dy_block, down_weight.T, preferred_element_type=jnp.float32)
        gate_f = gate_block.astype(jnp.float32)
        up_f = up_block.astype(jnp.float32)
        sigmoid_gate = jax.nn.sigmoid(gate_f)
        swish_gate = gate_f * sigmoid_gate
        hidden = (swish_gate * up_f).astype(jnp.bfloat16)
        gate_grad = (upstream * up_f * sigmoid_gate * (1.0 + gate_f * (1.0 - sigmoid_gate))).astype(jnp.bfloat16)
        up_grad = (upstream * swish_gate).astype(jnp.bfloat16)
        grad_split = up_grad.astype(jnp.float32).reshape(per_group, N_TENSOR, slices)
        partials = jnp.einsum("rkf,dkf->krd", grad_split, up_split, precision=lax.Precision.HIGHEST)
        rounded = lax.optimization_barrier(partials.astype(jnp.bfloat16)).astype(jnp.float32)
        input_grad = jnp.sum(rounded, axis=0).astype(jnp.bfloat16)
        accum = accum + jnp.dot(dy_block.T, hidden, preferred_element_type=jnp.float32)
        return accum, (input_grad, gate_grad)

    accum, outputs = lax.scan(one_group, jnp.zeros((D, FF), jnp.float32), (dy_blocks, gate_blocks, up_blocks))
    input_grads, gate_grads = outputs
    return input_grads.reshape(TOKENS, D), gate_grads.reshape(TOKENS, FF), accum / N_DP
```

```python
import jax
import jax.numpy as jnp
from jax import lax
from jax.sharding import PartitionSpec as P


COLUMNS = 2
CHUNKS = 2
LONGEST = 4

f32, bf16 = jnp.float32, jnp.bfloat16


def dot(a, b, dims):
    return lax.dot_general(a, b, (dims, ((), ())), preferred_element_type=f32)


def gathered(out_grad, gate_pre, up_pre, down_weight, up_weight):
    grad_rows = lax.all_gather(out_grad, "tensor", axis=0, tiled=True)
    gate_f, up_f = gate_pre.astype(f32), up_pre.astype(f32)
    sigmoid_gate = jax.nn.sigmoid(gate_f)
    swish_gate = gate_f * sigmoid_gate
    hidden = (swish_gate * up_f).astype(bf16)
    whole_down = lax.all_gather(down_weight, "dp", axis=1, tiled=True)
    whole_up = lax.all_gather(up_weight, "dp", axis=0, tiled=True)
    upstream = dot(grad_rows, whole_down, ((1,), (1,)))
    gate_grad = (upstream * up_f * sigmoid_gate * (1.0 + gate_f * (1.0 - sigmoid_gate))).astype(bf16)
    up_grad = (upstream * swish_gate).astype(bf16)
    partial = dot(up_grad, whole_up, ((1,), (1,))).astype(bf16)
    input_grad = lax.psum_scatter(partial, "tensor", scatter_dimension=0, tiled=True)
    product = dot(grad_rows, hidden, ((0,), (0,))) / lax.axis_size("dp")
    down_grad = lax.psum_scatter(product, "dp", scatter_dimension=0, tiled=True)
    return input_grad, gate_grad, down_grad


def shards(out_grad, gate_pre, up_pre, down_weight, up_weight):
    replicas, members = lax.axis_size("dp"), lax.axis_size("tensor")
    lines = replicas // COLUMNS
    place, member = lax.axis_index("dp"), lax.axis_index("tensor")
    spot, column = place // COLUMNS, place % COLUMNS
    own_rows, _ = out_grad.shape
    rows, hidden_units = gate_pre.shape
    share = up_weight.shape[0]
    pair = COLUMNS * share
    width = hidden_units // CHUNKS

    def chunk(a, axis, c):
        return lax.slice_in_dim(a, c * width, (c + 1) * width, axis=axis)

    def at(z, x):
        return z * COLUMNS + x

    def along(a, pairs):
        return lax.ppermute(a, "dp", [(at(i, x), at(j, x)) for i, j in pairs for x in range(COLUMNS)])

    def across(a):
        return lax.ppermute(a, "dp", [(at(z, x), at(z, 1 - x)) for z in range(lines) for x in range(COLUMNS)])

    def turn(a, k):
        return along(a, [(i, (i + k) % lines) for i in range(lines)])

    def swap(a, j):
        return lax.ppermute(a, "tensor", [(t, t ^ j) for t in range(members)])

    def piece(z):
        first = (z % lines) * pair
        return jnp.concatenate(
            [lax.dynamic_slice(out_grad, (0, first + x * share), (own_rows, share)) for x in (column, 1 - column)],
            axis=1,
        )

    other_down = across(down_weight)
    groups = {0: jnp.stack([piece(spot)] + [turn(piece(spot + k), k) for k in range(1, lines)])}
    j = members // 2
    while j:
        for have, value in list(groups.items()):
            groups[have ^ j] = swap(value, j)
        j //= 2
    all_groups = jnp.stack([groups[k] for k in range(members)])
    grads = jnp.stack(
        [lax.dynamic_index_in_dim(all_groups, member ^ t, 0, keepdims=False) for t in range(members)], axis=1
    ).reshape(lines, rows, pair)
    grads_left = lax.optimization_barrier(grads)

    other_up = across(up_weight)

    gate_f, up_f = gate_pre.astype(f32), up_pre.astype(f32)
    hidden = (gate_f * jax.nn.sigmoid(gate_f) * up_f).astype(bf16)
    back, ahead = [hidden], [hidden]
    for step in range(1, lines):
        back.append(along(back[-1], [(i, i + 1) for i in range(step - 1, lines - 1)]))
        ahead.append(along(ahead[-1], [(i + 1, i) for i in range(lines - step)]))

    weight = jnp.concatenate([down_weight, other_down], axis=1)
    gate_grads, up_grads = [], []
    for c in range(CHUNKS):
        w = chunk(weight, 0, c)
        r = l = None
        for step in range(1, lines):
            send_r = dot(grads[step], w, ((1,), (1,)))
            send_l = dot(grads_left[lines - step], w, ((1,), (1,)))
            if r is not None:
                send_r, send_l = send_r + r.astype(f32), send_l + l.astype(f32)
            r = along(send_r.astype(bf16), [(i, i + 1) for i in range(step)])
            l = along(send_l.astype(bf16), [(i, i - 1) for i in range(lines - step, lines)])
        upstream = dot(grads[0], w, ((1,), (1,))) + r.astype(f32) + l.astype(f32)
        g, u = chunk(gate_pre, 1, c).astype(f32), chunk(up_pre, 1, c).astype(f32)
        s = jax.nn.sigmoid(g)
        gate_grads.append((upstream * u * s * (1.0 + g * (1.0 - s))).astype(bf16))
        held = {0: (upstream * (g * s)).astype(bf16)}
        for k in range(1, lines // 2 + 1):
            held[k] = turn(held[k - 1], 1)
            if k < lines - k:
                held[lines - k] = turn(held[(lines - k + 1) % lines], lines - 1)
        up_grads.append(held)
        gate_pre, up_pre, _ = lax.optimization_barrier((gate_pre, up_pre, held[0]))
    gate_grad = jnp.concatenate(gate_grads, axis=1)

    line_hidden = jnp.concatenate([hidden] + [back[k] + ahead[lines - k] for k in range(1, lines)])
    both = grads.reshape(lines * rows, pair)
    mine, other = (
        dot(both[:, i * share : (i + 1) * share], line_hidden, ((0,), (0,))) / replicas for i in (0, 1)
    )
    from_pair = across(other.astype(bf16)).astype(f32)
    down_grad = mine + from_pair

    def product(k):
        return jnp.concatenate(
            [
                sum(dot(up_grads[c][k], chunk(w, 1, c), ((1,), (1,))) for c in range(CHUNKS)).astype(bf16)
                for w in (up_weight, other_up)
            ],
            axis=1,
        )

    done = {}
    for step in range(1, lines // 2 + 1):
        ks = sorted({step, lines - step}) + [0] * (step == 1)
        p = jnp.stack([product(k) for k in ks]).reshape(len(ks), members, own_rows, pair)

        def part_of(t):
            return lax.dynamic_index_in_dim(p, t, 1, keepdims=False)

        total = part_of(member).astype(f32)
        for j in range(1, members):
            total = total + swap(part_of(member ^ j), j).astype(f32)
        total = total.astype(bf16)
        for i, k in enumerate(ks):
            done[k] = turn(total[i], lines - k) if k else total[i]
    done = jnp.stack([done[k] for k in range(lines)])
    parts = []
    for z in range(lines):
        block = lax.dynamic_index_in_dim(done, (z - spot) % lines, 0, keepdims=False)
        first, second = block[:, :share], block[:, share:]
        parts += [jnp.where(column == 0, first, second), jnp.where(column == 0, second, first)]
    return jnp.concatenate(parts, axis=1), gate_grad, down_grad


def solution(mesh):
    placed = (
        P(("dp", "tensor"), None),
        P("dp", "tensor"),
        P("dp", "tensor"),
        P("tensor", "dp"),
        P("dp", "tensor"),
    )
    short = mesh.shape["dp"] <= LONGEST * COLUMNS

    def body(*args):
        return (shards if short else gathered)(*args)

    return jax.shard_map(
        body,
        mesh=mesh,
        in_specs=placed,
        out_specs=(P(("dp", "tensor"), None), P("dp", "tensor"), P("dp", "tensor")),
        check_vma=False,
    )
```

```python
import jax
import jax.numpy as jnp
from jax import lax
from jax.sharding import PartitionSpec as P


COLUMNS = 2
CHUNKS = 2
LINE = 4

f32, bf16 = jnp.float32, jnp.bfloat16


def dot(a, b, dims):
    return lax.dot_general(a, b, (dims, ((), ())), preferred_element_type=f32)


def gathered(out_grad, gate_pre, up_pre, down_weight, up_weight):
    grad_rows = lax.all_gather(out_grad, "tensor", axis=0, tiled=True)
    gate_f, up_f = gate_pre.astype(f32), up_pre.astype(f32)
    sigmoid_gate = jax.nn.sigmoid(gate_f)
    swish_gate = gate_f * sigmoid_gate
    hidden = (swish_gate * up_f).astype(bf16)
    whole_down = lax.all_gather(down_weight, "dp", axis=1, tiled=True)
    whole_up = lax.all_gather(up_weight, "dp", axis=0, tiled=True)
    upstream = dot(grad_rows, whole_down, ((1,), (1,)))
    gate_grad = (upstream * up_f * sigmoid_gate * (1.0 + gate_f * (1.0 - sigmoid_gate))).astype(bf16)
    up_grad = (upstream * swish_gate).astype(bf16)
    partial = dot(up_grad, whole_up, ((1,), (1,))).astype(bf16)
    input_grad = lax.psum_scatter(partial, "tensor", scatter_dimension=0, tiled=True)
    product = dot(grad_rows, hidden, ((0,), (0,))) / lax.axis_size("dp")
    down_grad = lax.psum_scatter(product, "dp", scatter_dimension=0, tiled=True)
    return input_grad, gate_grad, down_grad


def shards(out_grad, gate_pre, up_pre, down_weight, up_weight):
    replicas, members = lax.axis_size("dp"), lax.axis_size("tensor")
    lines = replicas // COLUMNS
    place, member = lax.axis_index("dp"), lax.axis_index("tensor")
    spot, column = place // COLUMNS, place % COLUMNS
    own_rows, _ = out_grad.shape
    rows, hidden_units = gate_pre.shape
    share = up_weight.shape[0]
    pair = COLUMNS * share
    width = hidden_units // CHUNKS

    def chunk(a, axis, c):
        return lax.slice_in_dim(a, c * width, (c + 1) * width, axis=axis)

    def at(z, x):
        return z * COLUMNS + x

    def along(a, pairs):
        return lax.ppermute(a, "dp", [(at(i, x), at(j, x)) for i, j in pairs for x in range(COLUMNS)])

    def across(a, places=None):
        places = range(lines) if places is None else places
        return lax.ppermute(a, "dp", [(at(z, x), at(z, 1 - x)) for z in places for x in range(COLUMNS)])

    def turn(a, k):
        return along(a, [(i, (i + k) % lines) for i in range(lines)])

    def swap(a, j):
        return lax.ppermute(a, "tensor", [(t, t ^ j) for t in range(members)])

    mates = [(z, z ^ 1) for z in range(lines)]
    inward, outward, middles = [(0, 1), (3, 2)], [(1, 0), (2, 3)], [(1, 2), (2, 1)]

    def piece(z):
        return jnp.concatenate(
            [lax.dynamic_slice(out_grad, (0, z * pair + x * share), (own_rows, share)) for x in (column, 1 - column)],
            axis=1,
        )

    other_down = across(down_weight)
    pieces = [piece(spot ^ k) for k in range(lines)]
    groups = {
        0: jnp.stack(pieces[:1] + [along(pieces[k], [(z, z ^ k) for z in range(lines)]) for k in range(1, lines)])
    }
    j = members // 2
    while j:
        for have, value in list(groups.items()):
            groups[have ^ j] = swap(value, j)
        j //= 2
    all_groups = jnp.stack([groups[k] for k in range(members)])
    grads = jnp.stack(
        [lax.dynamic_index_in_dim(all_groups, member ^ t, 0, keepdims=False) for t in range(members)], axis=1
    ).reshape(lines, rows, pair)

    grads_in = lax.optimization_barrier(grads)
    weight = jnp.concatenate([down_weight, other_down], axis=1)
    other_up = across(up_weight)

    gate_f, up_f = gate_pre.astype(f32), up_pre.astype(f32)
    hidden = (gate_f * jax.nn.sigmoid(gate_f) * up_f).astype(bf16)
    of_mate = along(hidden, mates)
    of_middle = along(hidden, middles)
    of_end = along(of_mate, middles)
    near, far = along(of_middle, outward), along(of_end, outward)
    line_hidden = jnp.concatenate([hidden, of_mate, of_end + near, of_middle + far])

    gate_grads, up_grads = [], []
    for c in range(CHUNKS):
        w = chunk(weight, 0, c)

        def times(a):
            return dot(a, w, ((1,), (1,)))

        for_end = along(times(grads_in[3]).astype(bf16), inward).astype(f32)
        for_middles = along(times(grads_in[1:3].reshape(2 * rows, pair)).astype(bf16), inward).astype(f32)
        far = along((times(grads[2]) + for_end).astype(bf16), middles).astype(f32)
        near = along((times(grads[3]) + for_middles[rows:]).astype(bf16), middles).astype(f32)
        came = along((times(grads[1]) + far).astype(bf16), outward).astype(f32)
        upstream = times(grads[0]) + came + near + for_middles[:rows]
        g, u = chunk(gate_pre, 1, c).astype(f32), chunk(up_pre, 1, c).astype(f32)
        s = jax.nn.sigmoid(g)
        gate_grads.append((upstream * u * s * (1.0 + g * (1.0 - s))).astype(bf16))
        held = {0: (upstream * (g * s)).astype(bf16)}
        for k in range(1, lines // 2 + 1):
            held[k] = turn(held[k - 1], 1)
            if k < lines - k:
                held[lines - k] = turn(held[(lines - k + 1) % lines], lines - 1)
        up_grads.append(held)
        gate_pre, up_pre, _ = lax.optimization_barrier((gate_pre, up_pre, held[0]))
    gate_grad = jnp.concatenate(gate_grads, axis=1)

    both = grads.reshape(lines * rows, pair)
    halves = [both[:, i * share : (i + 1) * share] for i in (0, 1)]
    other = dot(halves[1], line_hidden, ((0,), (0,))) / replicas
    mine = lax.optimization_barrier(dot(halves[0], line_hidden, ((0,), (0,))) / replicas)
    from_pair = across(other.astype(bf16)).astype(f32)
    down_grad = mine + from_pair

    both_up = jnp.concatenate([up_weight, other_up], axis=0)

    def product(k):
        return sum(dot(up_grads[c][k], chunk(both_up, 1, c), ((1,), (1,))) for c in range(CHUNKS)).astype(bf16)

    done = {}
    for step in range(1, lines // 2 + 1):
        ks = sorted({step, lines - step}) + [0] * (step == 1)
        p = jnp.stack([product(k) for k in ks]).reshape(len(ks), members, own_rows, pair)

        def part_of(t):
            return lax.dynamic_index_in_dim(p, t, 1, keepdims=False)

        total = part_of(member).astype(f32)
        for j in range(1, members):
            total = total + swap(part_of(member ^ j), j).astype(f32)
        total = total.astype(bf16)
        for i, k in enumerate(ks):
            done[k] = turn(total[i], lines - k) if k else total[i]
    parts = []
    for z in range(lines):
        block, ahead = done[0], (z - spot) % lines
        for k in range(1, lines):
            block = jnp.where(ahead == k, done[k], block)
        first, second = block[:, :share], block[:, share:]
        parts += [jnp.where(column == 0, first, second), jnp.where(column == 0, second, first)]
    return jnp.concatenate(parts, axis=1), gate_grad, down_grad


def solution(mesh):
    placed = (
        P(("dp", "tensor"), None),
        P("dp", "tensor"),
        P("dp", "tensor"),
        P("tensor", "dp"),
        P("dp", "tensor"),
    )
    short = mesh.shape["dp"] == LINE * COLUMNS

    def body(*args):
        return (shards if short else gathered)(*args)

    return jax.shard_map(
        body,
        mesh=mesh,
        in_specs=placed,
        out_specs=(P(("dp", "tensor"), None), P("dp", "tensor"), P("dp", "tensor")),
        check_vma=False,
    )
```

```python
import jax
import jax.numpy as jnp
from jax import lax
from jax.sharding import PartitionSpec as P


COLUMNS = 2
FIRST = 5
CHUNKS = 2
LINE = 4

f32, bf16 = jnp.float32, jnp.bfloat16


def dot(a, b, dims):
    return lax.dot_general(a, b, (dims, ((), ())), preferred_element_type=f32)


def gathered(out_grad, gate_pre, up_pre, down_weight, up_weight):
    grad_rows = lax.all_gather(out_grad, "tensor", axis=0, tiled=True)
    gate_f, up_f = gate_pre.astype(f32), up_pre.astype(f32)
    sigmoid_gate = jax.nn.sigmoid(gate_f)
    swish_gate = gate_f * sigmoid_gate
    hidden = (swish_gate * up_f).astype(bf16)
    whole_down = lax.all_gather(down_weight, "dp", axis=1, tiled=True)
    whole_up = lax.all_gather(up_weight, "dp", axis=0, tiled=True)
    upstream = dot(grad_rows, whole_down, ((1,), (1,)))
    gate_grad = (upstream * up_f * sigmoid_gate * (1.0 + gate_f * (1.0 - sigmoid_gate))).astype(bf16)
    up_grad = (upstream * swish_gate).astype(bf16)
    partial = dot(up_grad, whole_up, ((1,), (1,))).astype(bf16)
    input_grad = lax.psum_scatter(partial, "tensor", scatter_dimension=0, tiled=True)
    product = dot(grad_rows, hidden, ((0,), (0,))) / lax.axis_size("dp")
    down_grad = lax.psum_scatter(product, "dp", scatter_dimension=0, tiled=True)
    return input_grad, gate_grad, down_grad


def shards(out_grad, gate_pre, up_pre, down_weight, up_weight):
    replicas, members = lax.axis_size("dp"), lax.axis_size("tensor")
    lines = replicas // COLUMNS
    place, member = lax.axis_index("dp"), lax.axis_index("tensor")
    spot, column = place // COLUMNS, place % COLUMNS
    own_rows, _ = out_grad.shape
    rows, hidden_units = gate_pre.shape
    share = up_weight.shape[0]
    pair = COLUMNS * share
    first = hidden_units * FIRST // 128 // 14 * 128
    bounds = (0, first, hidden_units)

    def chunk(a, axis, c):
        return lax.slice_in_dim(a, bounds[c], bounds[c + 1], axis=axis)

    def at(z, x):
        return z * COLUMNS + x

    def along(a, pairs):
        return lax.ppermute(a, "dp", [(at(i, x), at(j, x)) for i, j in pairs for x in range(COLUMNS)])

    def across(a, places=None):
        places = range(lines) if places is None else places
        return lax.ppermute(a, "dp", [(at(z, x), at(z, 1 - x)) for z in places for x in range(COLUMNS)])

    def turn(a, k):
        return along(a, [(i, (i + k) % lines) for i in range(lines)])

    def swap(a, j):
        return lax.ppermute(a, "tensor", [(t, t ^ j) for t in range(members)])

    mates = [(z, z ^ 1) for z in range(lines)]
    inward, outward, middles = [(0, 1), (3, 2)], [(1, 0), (2, 3)], [(1, 2), (2, 1)]

    def piece(z):
        return jnp.concatenate(
            [lax.dynamic_slice(out_grad, (0, z * pair + x * share), (own_rows, share)) for x in (column, 1 - column)],
            axis=1,
        )

    other_down = across(down_weight)
    pieces = [piece(spot ^ k) for k in range(lines)]
    groups = {
        0: jnp.stack(pieces[:1] + [along(pieces[k], [(z, z ^ k) for z in range(lines)]) for k in range(1, lines)])
    }
    j = members // 2
    while j:
        for have, value in list(groups.items()):
            groups[have ^ j] = swap(value, j)
        j //= 2
    all_groups = jnp.stack([groups[k] for k in range(members)])
    grads = jnp.stack(
        [lax.dynamic_index_in_dim(all_groups, member ^ t, 0, keepdims=False) for t in range(members)], axis=1
    ).reshape(lines, rows, pair)

    grads_in = lax.optimization_barrier(grads)
    weight = jnp.concatenate([down_weight, other_down], axis=1)
    other_up = across(up_weight)

    gate_f, up_f = gate_pre.astype(f32), up_pre.astype(f32)
    hidden = (gate_f * jax.nn.sigmoid(gate_f) * up_f).astype(bf16)
    of_mate = along(hidden, mates)
    of_middle = along(hidden, middles)
    of_end = along(of_mate, middles)
    near, far = along(of_middle, outward), along(of_end, outward)
    line_hidden = jnp.concatenate([hidden, of_mate, of_end + near, of_middle + far])

    gate_grads, up_grads = [], []
    for c in range(CHUNKS):
        w = chunk(weight, 0, c)

        def times(a):
            return dot(a, w, ((1,), (1,)))

        for_end = along(times(grads_in[3]).astype(bf16), inward).astype(f32)
        for_middles = along(times(grads_in[1:3].reshape(2 * rows, pair)).astype(bf16), inward).astype(f32)
        far = along((times(grads[2]) + for_end).astype(bf16), middles).astype(f32)
        near = along((times(grads[3]) + for_middles[rows:]).astype(bf16), middles).astype(f32)
        came = along((times(grads[1]) + far).astype(bf16), outward).astype(f32)
        upstream = times(grads[0]) + came + near + for_middles[:rows]
        g, u = chunk(gate_pre, 1, c).astype(f32), chunk(up_pre, 1, c).astype(f32)
        s = jax.nn.sigmoid(g)
        gate_grads.append((upstream * u * s * (1.0 + g * (1.0 - s))).astype(bf16))
        held = {0: (upstream * (g * s)).astype(bf16)}
        for k in range(1, lines // 2 + 1):
            held[k] = turn(held[k - 1], 1)
            if k < lines - k:
                held[lines - k] = turn(held[(lines - k + 1) % lines], lines - 1)
        up_grads.append(held)
        gate_pre, up_pre, _ = lax.optimization_barrier((gate_pre, up_pre, held[0]))
    gate_grad = jnp.concatenate(gate_grads, axis=1)

    both = grads.reshape(lines * rows, pair)
    halves = [both[:, i * share : (i + 1) * share] for i in (0, 1)]
    other = dot(halves[1], line_hidden, ((0,), (0,))) / replicas
    mine = lax.optimization_barrier(dot(halves[0], line_hidden, ((0,), (0,))) / replicas)
    from_pair = across(other.astype(bf16)).astype(f32)
    down_grad = mine + from_pair

    both_up = jnp.concatenate([up_weight, other_up], axis=0)

    def product(k):
        return sum(dot(up_grads[c][k], chunk(both_up, 1, c), ((1,), (1,))) for c in range(CHUNKS)).astype(bf16)

    done = {}
    for step in range(1, lines // 2 + 1):
        ks = sorted({step, lines - step}) + [0] * (step == 1)
        p = jnp.stack([product(k) for k in ks]).reshape(len(ks), members, own_rows, pair)

        def part_of(t):
            return lax.dynamic_index_in_dim(p, t, 1, keepdims=False)

        total = part_of(member).astype(f32)
        for j in range(1, members):
            total = total + swap(part_of(member ^ j), j).astype(f32)
        total = total.astype(bf16)
        for i, k in enumerate(ks):
            done[k] = turn(total[i], lines - k) if k else total[i]
    parts = []
    for z in range(lines):
        block, ahead = done[0], (z - spot) % lines
        for k in range(1, lines):
            block = jnp.where(ahead == k, done[k], block)
        first, second = block[:, :share], block[:, share:]
        parts += [jnp.where(column == 0, first, second), jnp.where(column == 0, second, first)]
    return jnp.concatenate(parts, axis=1), gate_grad, down_grad


def solution(mesh):
    placed = (
        P(("dp", "tensor"), None),
        P("dp", "tensor"),
        P("dp", "tensor"),
        P("tensor", "dp"),
        P("dp", "tensor"),
    )
    short = mesh.shape["dp"] == LINE * COLUMNS

    def body(*args):
        return (shards if short else gathered)(*args)

    return jax.shard_map(
        body,
        mesh=mesh,
        in_specs=placed,
        out_specs=(P(("dp", "tensor"), None), P("dp", "tensor"), P("dp", "tensor")),
        check_vma=False,
    )
```
